256 devices in a mesh: wrow: 32 (over y, x, z_lo), kblk: 8 (over z_hi, core).
Axes of the slice: x: 4, y: 4, z: 8 (z_hi: 4, z_lo: 2; z = z_hi * 2 + z_lo), core: 2. Of those that a mesh axis runs over, the one named last changes fastest.
Arguments:
- conduction: bfloat16 [8, 4, 64, 16384], P('kblk', None, None, 'wrow'), may hold values from -6 to 6
- valence: bfloat16 [8, 4, 64, 16384], P(None, None, 'wrow', 'kblk'), may hold values from -6 to 6
- screened: bfloat16 [4, 16384, 16384], P(None, 'wrow', 'kblk'), may hold values from -0.00036621094 to 0.00036621094
- pair_block: int32 [8, 4], replicated, may hold values from 0 to 3, as said below
Outputs:
- kernel: float32 [8, 64, 256], P('kblk', 'wrow')
The draws below stay inside these ranges and needn't reach their ends.
Inputs may be any that keep to these rules, and one draw needn't show every extreme that they name: `pair_block`: every one of the 4 blocks is selected by at least one pair and by at most 12 pairs; one block by exactly 12 pairs.
All inputs are finite; a program needn't handle non-finite values.
Results may differ from the reference program's by a relative error of at most 0.0029.
Values may be sent and summed in bfloat16 or wider, within the bound.
A program may use at most 128 MiB of HBM per device.

```python
import jax
import jax.numpy as jnp
from jax import lax

NG = 16384
C = 8
V = 8
KP = 4
NQ = 4
NK = 8
CAP = 12
SLAB = 2048


def draw_pair_block(key, part):
    total = NK * KP
    key_full = jax.random.fold_in(key, 11)
    key_shift = jax.random.fold_in(key, 12)
    key_perm = jax.random.fold_in(key, 13)
    full_block = jax.random.randint(key_full, (), 0, NQ)
    shift = jax.random.randint(key_shift, (), 0, NQ - 1)
    positions = jnp.arange(total, dtype=jnp.int32)
    others = (positions - CAP + shift) % (NQ - 1)
    others = jnp.where(others >= full_block, others + 1, others)
    labels = jnp.where(positions < CAP, full_block, others)
    labels = jax.random.permutation(key_perm, labels)
    return labels.reshape(NK, KP).astype(jnp.int32)


def block_levels(key, shape, shards, low, high):
    def one(position, parts):
        draws = jax.random.uniform(jax.random.fold_in(jax.random.fold_in(key, 6), position), (parts,), jnp.float32, low / len(shards), high / len(shards))
        return jnp.repeat(jnp.exp(draws), shape[position] // parts).reshape((-1,) + (1,) * (len(shape) - position - 1))

    factor_of = one(*shards[0])
    for cut in shards[1:]:
        factor_of = factor_of * one(*cut)
    return factor_of


def centred(stream_key, shape, deviation, reach, pieces=(), kind=jnp.bfloat16):
    drawn = jax.random.normal(stream_key, shape, jnp.float32) * deviation
    if len(pieces) > 0:
        drawn = block_levels(stream_key, shape, pieces, -0.22, 0.18) * drawn
    return jnp.clip(drawn, min=-reach, max=reach).astype(kind)


def setup_inputs(seed: int = 0) -> dict:
    keys = jax.random.split(jax.random.key(seed), 5)
    conduction = centred(keys[0], (NK, KP, C * C, NG), 1.0, 6.0, ((0, 8), (3, 32)))
    valence = centred(keys[1], (NK, KP, V * V, NG), 1.0, 6.0, ((2, 32), (3, 8)))
    screened = centred(keys[2], (NQ, NG, NG), (NG * NG) ** -0.5, 0.00036621094, ((1, 32), (2, 8)))
    pair_block = draw_pair_block(jax.random.fold_in(keys[4], 71), 0)
    return dict(conduction=conduction, valence=valence, screened=screened, pair_block=pair_block)


def reference(conduction, valence, screened, pair_block):
    pair_count = NK * KP
    cond_rows = conduction.reshape(pair_count, C * C, NG)
    vale_rows = valence.reshape(pair_count, V * V, NG)
    blocks = pair_block.reshape(pair_count).astype(jnp.int32)
    slab_count = NG // SLAB

    def one_pair(items):
        cond_one, vale_one, block = items
        w_full = lax.dynamic_index_in_dim(screened, block, 0, keepdims=False)

        def one_slab(total, slab):
            start = (slab * SLAB).astype(jnp.int32)
            w_cols = lax.dynamic_slice_in_dim(w_full, start, SLAB, 1)
            v_cols = lax.dynamic_slice_in_dim(vale_one, start, SLAB, 1)
            part = jnp.dot(v_cols, w_cols.T, preferred_element_type=jnp.float32).astype(jnp.bfloat16)
            return total + jnp.dot(cond_one, part.T, preferred_element_type=jnp.float32), None

        total, _ = lax.scan(one_slab, jnp.zeros((C * C, V * V), jnp.float32), jnp.arange(slab_count, dtype=jnp.int32))
        return total

    tiles = lax.map(one_pair, (cond_rows, vale_rows, blocks))
    tiles = tiles.reshape(NK, KP, C, C, V, V).transpose(0, 2, 4, 1, 3, 5)
    return tiles.reshape(NK, C * V, KP * C * V)
```

```python
import functools

import jax
import jax.numpy as jnp
from jax import lax
from jax.experimental import pallas as pl
from jax.experimental.pallas import tpu as pltpu
from jax.sharding import Mesh
from jax.sharding import PartitionSpec as P

AXES = ("py", "px", "zl", "zh", "core")
WROW = ("py", "px", "zl")
KBLK = ("zh", "core")
MESH = pl.DeviceIdType.MESH
DMA = pltpu.SemaphoreType.DMA


def kernel(vale, cond, screened, ql, out,
           vbuf, cbuf, wbuf, xacc, xhold, zs, zrecv, total, r1buf, t1, r2buf,
           lsem, ssem, rsem, cssem, crsem, dsem, r1s, r1r, r2s, r2r):
    py, px, zl, zh, core = (lax.axis_index(a) for a in AXES)
    me = dict(py=py, px=px, zl=zl, zh=zh, core=core)

    def at(**moved):
        return tuple(moved.get(a, me[a]) for a in AXES)

    def mod4(v):
        return lax.rem(v + 8, 4)

    own_k = zh * 2 + core
    first = ("px", "py")
    second = ("py", "px")

    def slot(h, d1, d2, zz):
        return (h, mod4(me[second[h]] + d2), mod4(me[first[h]] + d1), lax.rem(zl + zz, 2))

    locals_ = []
    for h in range(2):
        locals_.append(pltpu.make_async_copy(vale.at[h], vbuf.at[slot(h, 0, 0, 0)], lsem.at[h]))
    locals_.append(pltpu.make_async_copy(cond, cbuf.at[own_k], lsem.at[2]))
    locals_.append(pltpu.make_async_copy(screened, wbuf, lsem.at[3]))
    for c in locals_:
        c.start()

    barrier = pltpu.get_barrier_semaphore()
    for dy in range(4):
        for dx in range(4):
            if dx or dy:
                pl.semaphore_signal(barrier, inc=1, device_id=at(py=mod4(py + dy), px=mod4(px + dx)),
                                    device_id_type=MESH)
    for dl in range(2):
        for dh in range(4):
            for dc in range(2):
                if dl or dh or dc:
                    pl.semaphore_signal(
                        barrier, inc=1,
                        device_id=at(zl=lax.rem(zl + dl, 2), zh=mod4(zh + dh), core=lax.rem(core + dc, 2)),
                        device_id_type=MESH)
    for c in locals_[:3]:
        c.wait()
    pl.semaphore_wait(barrier, 30)

    started = []

    def send(src, dst, s, r, to):
        c = pltpu.make_async_remote_copy(src_ref=src, dst_ref=dst, send_sem=s, recv_sem=r,
                                         device_id=to, device_id_type=MESH)
        c.start()
        started.append(c)

    counts = [0, 0]

    def vsend(h, chunk, axis, step):
        d1, d2, zz = chunk
        ref = vbuf.at[slot(h, d1, d2, zz)]
        if axis == "zl":
            to, r = at(zl=1 - zl), (h, 0, 0, 1)
        else:
            to = at(**{axis: mod4(me[axis] + step)})
            r = ((h, d2 % 4, (d1 - step) % 4, zz) if axis == first[h] else (h, (d2 - step) % 4, d1 % 4, zz))
        send(ref, ref, ssem.at[h, counts[h]], rsem.at[r], to)
        counts[h] += 1

    def vwait(h, chunk):
        d1, d2, zz = chunk
        ref = vbuf.at[slot(h, d1, d2, zz)]
        sem = rsem.at[h, d2 % 4, d1 % 4, zz]
        pltpu.make_async_remote_copy(src_ref=ref, dst_ref=ref, send_sem=sem, recv_sem=sem,
                                     device_id=at(core=1 - core), device_id_type=MESH).wait_recv()

    def phase1(h, chunk):
        d1, _, zz = chunk
        if d1 == 0:
            vsend(h, chunk, first[h], 1)
            vsend(h, chunk, first[h], -1)
        if d1 == -1 and zz == 0:
            vsend(h, chunk, first[h], 1)
        if d1 == 1 and zz == 1:
            vsend(h, chunk, first[h], -1)

    def phase2(h, chunk):
        vsend(h, chunk, second[h], 1)
        vsend(h, chunk, second[h], -1)

    def csend(o):
        send(cbuf.at[own_k], cbuf.at[own_k], cssem.at[o], crsem.at[o], at(zh=mod4(zh + o)))

    def partner(o):
        ref = cbuf.at[mod4(zh - o) * 2 + core]
        send(ref, ref, cssem.at[4 + o], crsem.at[4 + o], at(core=1 - core))

    def cwait(o, far):
        ref = cbuf.at[mod4(zh - o) * 2 + (1 - core if far else core)]
        sem = crsem.at[(4 if far else 0) + o]
        pltpu.make_async_remote_copy(src_ref=ref, dst_ref=ref, send_sem=sem, recv_sem=sem,
                                     device_id=at(core=1 - core), device_id_type=MESH).wait_recv()

    own = (0, 0, 0)
    for h in range(2):
        vsend(h, own, "zl", 1)
    for h in range(2):
        phase1(h, own)
    partner(0)
    for h in range(2):
        phase2(h, own)
    for o in (1, 3, 2):
        csend(o)

    for chunks in (((0, 0, 1),), ((-1, 0, 0), (1, 0, 0)), ((-1, 0, 1), (1, 0, 1)), ((2, 0, 0), (2, 0, 1))):
        for chunk in chunks:
            for h in range(2):
                vwait(h, chunk)
                phase1(h, chunk)
                phase2(h, chunk)
    locals_[3].wait()

    lane = lax.broadcasted_iota(jnp.int32, (64, 256), 1)
    pair_of_lane = lax.rem(lax.div(lane, 2), 16)

    def stage1(h, d2):
        a2 = mod4(me[second[h]] + d2)
        block_of_lane = ql[h][0:1]

        @pl.loop(0, 4)
        def _(q):
            v = vbuf[h, a2].reshape(256, 2048)
            x = lax.dot_general(wbuf[q], v, (((1,), (1,)), ((), ())), preferred_element_type=jnp.float32)
            chosen = jnp.broadcast_to(block_of_lane == q, x.shape)
            xacc[...] = jnp.where(jnp.logical_or(chosen, q == 0), x, xacc[...])

    def stage2(h, d2, x):
        a2 = mod4(me[second[h]] + d2)
        z = jnp.zeros((64, 256), jnp.float32)
        for kk in range(4):
            y = jnp.dot(cbuf[4 * h + kk].reshape(256, 512), x, preferred_element_type=jnp.float32)
            for kp in range(4):
                z = jnp.where(pair_of_lane == kk * 4 + kp, y[kp * 64:kp * 64 + 64], z)
        for half in range(2):
            tile = z[:, half * 128:half * 128 + 128].reshape(8, 8, 128)
            if h == 0:
                zs[0, lax.div(a2, 2), :, lax.rem(a2, 2) * 2 + half] = tile
            else:
                zs[1, half, :, a2] = tile

    for h in range(2):
        stage1(h, 0)
        xhold[h] = xacc[...].astype(jnp.bfloat16)

    def forward(d1):
        for zz in range(2):
            for h in range(2):
                for d2 in (-1, 1):
                    chunk = (d1, d2, zz)
                    vwait(h, chunk)
                    if d2 == -1 and zz == 0:
                        vsend(h, chunk, second[h], 1)
                    if d2 == 1 and zz == 1:
                        vsend(h, chunk, second[h], -1)

    forward(0)
    cwait(0, True)
    for o in (1, 3, 2):
        cwait(o, False)
        partner(o)
    for o in (1, 3, 2):
        cwait(o, True)
    forward(-1)
    for h in range(2):
        stage2(h, 0, xhold[h])
    for d1 in (1, 2):
        forward(d1)
    for d2 in (-1, 1):
        for h in range(2):
            stage1(h, d2)
            stage2(h, d2, xacc[...].astype(jnp.bfloat16))
    for h in range(2):
        for d1 in (0, -1, 1, 2):
            for zz in range(2):
                vwait(h, (d1, 2, zz))
        stage1(h, 2)
        stage2(h, 2, xacc[...].astype(jnp.bfloat16))

    send(zs.at[1 - core], zrecv, dsem.at[0], dsem.at[1], at(core=1 - core))
    started.pop().wait()
    total[...] = zs[core] + zrecv[...]

    offsets = [(dy, dx) for dy in range(4) for dx in range(4) if dx or dy]
    for dy, dx in offsets:
        ty, tx = mod4(py + dy), mod4(px + dx)
        i = dy * 4 + dx
        send(total.at[lax.rem(tx, 2), ty * 2 + lax.div(tx, 2)], r1buf.at[i], r1s.at[i], r1r.at[i], at(py=ty, px=tx))
    acc = total[lax.rem(px, 2), py * 2 + lax.div(px, 2)]
    for dy, dx in offsets:
        i = dy * 4 + dx
        pltpu.make_async_remote_copy(src_ref=r1buf.at[i], dst_ref=r1buf.at[i], send_sem=r1s.at[i], recv_sem=r1r.at[i],
                                     device_id=at(core=1 - core), device_id_type=MESH).wait_recv()
        acc = acc + r1buf[i]
    t1[...] = acc

    here = zl * 4 + zh
    for tl in range(2):
        for th in range(2):
            for tc in range(2):
                i = tl * 4 + th * 2 + tc
                dest = at(zl=tl, zh=core * 2 + th, core=tc)
                mine = jnp.logical_and(jnp.logical_and(zl == tl, core == tc), zh == core * 2 + th)
                copy = pltpu.make_async_remote_copy(src_ref=t1, dst_ref=r2buf.at[here], send_sem=r2s.at[i],
                                                    recv_sem=r2r.at[here], device_id=dest, device_id_type=MESH)

                @pl.when(jnp.logical_not(mine))
                def _():
                    copy.start()

                @pl.when(mine)
                def _():
                    r2buf[here] = acc

    for i in range(8):
        mine = jnp.logical_and(lax.div(zh, 2) == core, here == i)

        @pl.when(jnp.logical_not(mine))
        def _():
            pltpu.make_async_remote_copy(src_ref=t1, dst_ref=r2buf.at[i], send_sem=r2s.at[i], recv_sem=r2r.at[i],
                                         device_id=at(core=1 - core), device_id_type=MESH).wait_recv()

    acc = r2buf[0]
    for i in range(1, 8):
        acc = acc + r2buf[i]
    out[...] = acc

    for c in started:
        c.wait_send()
    for tl in range(2):
        for th in range(2):
            for tc in range(2):
                i = tl * 4 + th * 2 + tc
                mine = jnp.logical_and(jnp.logical_and(zl == tl, core == tc), zh == core * 2 + th)

                @pl.when(jnp.logical_not(mine))
                def _():
                    pltpu.make_async_remote_copy(src_ref=t1, dst_ref=t1, send_sem=r2s.at[i], recv_sem=r2r.at[i],
                                                 device_id=at(core=1 - core), device_id_type=MESH).wait_send()


def per_device(conduction, valence, screened, pair_block):
    vale = valence.reshape(2, 32, 2048)
    cond = conduction.reshape(4, 64, 512)
    pairs = pair_block.reshape(2, 1, 1, 16, 1)
    ql = jnp.broadcast_to(pairs, (2, 8, 8, 16, 2)).reshape(2, 8, 256)
    part = pl.pallas_call(
        kernel,
        out_shape=jax.ShapeDtypeStruct((4, 8, 128), jnp.float32),
        in_specs=[pl.BlockSpec(memory_space=pl.ANY)] * 3 + [pl.BlockSpec(memory_space=pltpu.VMEM)],
        out_specs=pl.BlockSpec(memory_space=pltpu.VMEM),
        scratch_shapes=[
            pltpu.VMEM((2, 4, 4, 2, 32, 2048), jnp.bfloat16),
            pltpu.VMEM((8, 4, 64, 512), jnp.bfloat16),
            pltpu.VMEM((4, 512, 2048), jnp.bfloat16),
            pltpu.VMEM((512, 256), jnp.float32),
            pltpu.VMEM((2, 512, 256), jnp.bfloat16),
            pltpu.VMEM((2, 2, 8, 4, 8, 128), jnp.float32),
            pltpu.VMEM((2, 8, 4, 8, 128), jnp.float32),
            pltpu.VMEM((2, 8, 4, 8, 128), jnp.float32),
            pltpu.VMEM((16, 4, 8, 128), jnp.float32),
            pltpu.VMEM((4, 8, 128), jnp.float32),
            pltpu.VMEM((8, 4, 8, 128), jnp.float32),
            DMA((4,)),
            DMA((2, 31)),
            DMA((2, 4, 4, 2)),
            DMA((8,)),
            DMA((8,)),
            DMA((2,)),
            DMA((16,)),
            DMA((16,)),
            DMA((8,)),
            DMA((8,)),
        ],
        compiler_params=pltpu.CompilerParams(collective_id=0, has_side_effects=True,
                                             vmem_limit_bytes=48 * 1024 * 1024),
    )(vale, cond, screened, ql)
    zl, zh, core = (lax.axis_index(a) for a in ("zl", "zh", "core"))
    kk = lax.rem(zh, 2) * 2 + core
    lo = part.reshape(2, 2, 8, 2, 2, 4, 4, 2)
    lo = lax.dynamic_index_in_dim(lo, zl, 0, False)
    lo = lax.dynamic_index_in_dim(lo, kk, 4, False)
    lo = lo.transpose(0, 4, 1, 2, 3, 5)
    hi = part.reshape(2, 2, 8, 2, 2, 4, 4, 2)
    hi = lax.dynamic_index_in_dim(hi, zl, 3, False)
    hi = lax.dynamic_index_in_dim(hi, kk, 4, False)
    hi = hi.transpose(0, 4, 2, 1, 3, 5)
    return jnp.where(zh < 2, lo.reshape(1, 2, 256), hi.reshape(1, 2, 256))


def solution(mesh):
    finer = Mesh(mesh.devices.reshape(4, 4, 2, 4, 2), AXES)
    return jax.shard_map(
        per_device,
        mesh=finer,
        in_specs=(P(KBLK, None, None, WROW), P(None, None, WROW, KBLK), P(None, WROW, KBLK), P()),
        out_specs=P(KBLK, WROW, None),
        check_vma=False,
    )
```
